32 devices in a mesh: row: 8 (over y, x, core), col: 4 (over z).
Axes of the slice: x: 2, y: 2, z: 4, core: 2. Of those that a mesh axis runs over, the one named last changes fastest.
Arguments:
- pair_factors: float32 [12288, 1024], P(('row', 'col')), may hold values from -0.09375 to 0.09375
- k_prev: float32 [12288, 12288], P('row', 'col'), as said below
- energies: float32 [12288], P('row'), may hold values from 0.3 to 2
Outputs:
- casida: float32 [12288, 12288], P('row', 'col')
- vectors: float32 [12288, 8], P('row')
- images: float32 [12288, 8], P('row')
- tridiagonal: float32 [2, 8], replicated
The draws below stay inside these ranges and needn't reach their ends.
Inputs may be any that keep to these rules, and one draw needn't show every extreme that they name: k_prev is exactly symmetric.
All inputs are finite; a program needn't handle non-finite values.
Results may differ from the reference program's by a relative error of at most 0.0003.
Values sent between devices are 32-bit elements; how exact they have to be, the bound alone decides.
A program may use at most 128 MiB of HBM per device.

```python
import math
import jax
import jax.numpy as jnp
from jax import lax

N = 12288
PC = 8
AUXW = 1024


def draw_k_prev(key, part):
    base = 0.02 * jax.random.normal(key, (N, N), jnp.float32)
    return (base + base.T) * 0.7071


def shard_levels(key, extent, split, low, largest):
    factor_of, own = 1.0, jax.random.fold_in(key, 6)
    for position, shards_of in split:
        heights = jnp.exp(jax.random.uniform(jax.random.fold_in(own, position), (shards_of,), jnp.float32, low / len(split), largest / len(split)))
        factor_of = factor_of * jnp.repeat(heights, extent[position] // shards_of).reshape([-1 if axis == position else 1 for axis in range(len(extent))])
    return factor_of


def scatter_about(stream_key, shape, spread, limit, cuts=(), kind=jnp.bfloat16):
    drawn = jax.random.normal(stream_key, shape, jnp.float32) * spread
    if len(cuts) > 0:
        drawn = shard_levels(stream_key, shape, cuts, -0.22, 0.18) * drawn
    return jnp.clip(drawn, min=-limit, max=limit).astype(kind)


def setup_inputs(seed: int = 0) -> dict:
    seeds = jax.random.split(jax.random.key(seed), 4)
    pair_factors = scatter_about(seeds[0], (N, AUXW), (0.5 * AUXW ** -0.5), 0.09375, ((0, 32),), jnp.float32)
    k_prev = draw_k_prev(jax.random.fold_in(seeds[3], 71), 0)
    energies = jnp.clip(jnp.exp(math.log(2.0) - 1.89712 * jax.random.uniform(seeds[2], (N,), jnp.float32) ** shard_levels(seeds[2], (N,), ((0, 8),), -0.2, 0.2)), 0.3, 2.0)
    return {"pair_factors": pair_factors, "k_prev": k_prev, "energies": energies}


def reference(pair_factors, k_prev, energies):
    coupling = k_prev + jnp.dot(pair_factors, pair_factors.T, precision=lax.Precision.HIGHEST, preferred_element_type=jnp.float32)
    casida = 4.0 * coupling + jnp.diag(energies)
    row_ids = jnp.arange(N, dtype=jnp.int32)
    col_ids = jnp.arange(PC, dtype=jnp.int32)
    upper = jnp.zeros((N, PC), jnp.float32)
    lower = jnp.zeros((N, PC), jnp.float32)
    diag_list = []
    sub_list = []
    for column_at in range(PC):
        column = casida[:, column_at] - jnp.dot(upper, lower[column_at], precision=lax.Precision.HIGHEST) - jnp.dot(lower, upper[column_at], precision=lax.Precision.HIGHEST)
        diag_list.append(column[column_at])
        below = jnp.where(row_ids > column_at, column, 0.0)
        lead = column[column_at + 1]
        sigma = jnp.sum(below * below)
        root = jnp.sqrt(sigma)
        alpha = jnp.where(lead >= 0, -root, root)
        vector = below - alpha * (row_ids == column_at + 1).astype(jnp.float32)
        length = jnp.sqrt(jnp.maximum(2.0 * (sigma + jnp.abs(lead) * root), 1.0))
        unit = vector / length
        image = jnp.dot(casida, unit, precision=lax.Precision.HIGHEST)
        image = image - jnp.dot(upper, jnp.dot(lower.T, unit, precision=lax.Precision.HIGHEST), precision=lax.Precision.HIGHEST)
        image = image - jnp.dot(lower, jnp.dot(upper.T, unit, precision=lax.Precision.HIGHEST), precision=lax.Precision.HIGHEST)
        image = 2.0 * image
        partner = image - jnp.sum(image * unit) * unit
        pick = (col_ids == column_at).astype(jnp.float32)[None, :]
        upper = upper + unit[:, None] * pick
        lower = lower + partner[:, None] * pick
        sub_list.append(alpha)
    scale = jnp.sqrt(jnp.float32(N))
    tridiagonal = jnp.stack([jnp.stack(diag_list), jnp.stack(sub_list)])
    return (casida, scale * upper, scale * lower, tridiagonal)
```

```python
import functools

import jax
import jax.numpy as jnp
from jax import lax
from jax.experimental import pallas as pl
from jax.experimental.pallas import tpu as pltpu
from jax.sharding import PartitionSpec as P

PC = 8
LANES = 128
MESH = pl.DeviceIdType.MESH
HIGHEST = lax.Precision.HIGHEST


def panel_kernel(
    n_row, n_col, part_ref, casida_ref, upper_out, lower_out, tri_out,
    block, panel_in, panel, upper, lower, unit, sums, mine, whole_row, from_col, from_row,
    load_sem, own_sem, pa_send, pa_recv, pb_send, pb_recv, c_send, c_recv, r_send, r_recv,
):
    r = lax.axis_index("row")
    c = lax.axis_index("col")
    rows_here, cols_here = block.shape
    total = n_row * rows_here
    load = pltpu.make_async_copy(casida_ref, block, load_sem)
    load.start()
    col_peers = [lax.rem(c + d, n_col) for d in range(1, n_col)]
    row_peers = [lax.rem(r + d, n_row) for d in range(1, n_row)]
    barrier = pltpu.get_barrier_semaphore()
    for peer in col_peers:
        pl.semaphore_signal(barrier, inc=1, device_id=(r, peer), device_id_type=MESH)
    for peer in row_peers:
        pl.semaphore_signal(barrier, inc=1, device_id=(peer, c), device_id_type=MESH)
    pl.semaphore_wait(barrier, n_col + n_row - 2)

    @pl.when(r == 0)
    def _():
        own = pltpu.make_async_copy(part_ref, panel_in.at[c], own_sem)
        own.start()
        copies = [
            pltpu.make_async_remote_copy(
                part_ref, panel_in.at[c], pa_send.at[d - 1], pa_recv,
                device_id=(jnp.int32(d), c), device_id_type=MESH,
            )
            for d in range(1, n_row)
        ]
        for copy in copies:
            copy.start()
        for copy in copies:
            copy.wait_send()
        own.wait()

    @pl.when(r != 0)
    def _():
        pltpu.make_async_remote_copy(
            part_ref, panel_in.at[c], pa_send.at[0], pa_recv,
            device_id=(jnp.int32(0), c), device_id_type=MESH,
        ).wait_recv()

    copies = [
        pltpu.make_async_remote_copy(
            panel_in.at[c], panel_in.at[c], pb_send.at[i], pb_recv.at[c],
            device_id=(r, peer), device_id_type=MESH,
        )
        for i, peer in enumerate(col_peers)
    ]
    for copy in copies:
        copy.start()
    for peer in col_peers:
        pltpu.make_async_remote_copy(
            panel_in.at[peer], panel_in.at[peer], pb_send.at[0], pb_recv.at[peer],
            device_id=(r, peer), device_id_type=MESH,
        ).wait_recv()
    for copy in copies:
        copy.wait_send()
    for k in range(n_col):
        panel[:, k * cols_here:(k + 1) * cols_here] = panel_in[k]
    upper[...] = jnp.zeros_like(upper)
    lower[...] = jnp.zeros_like(lower)
    tri_out[...] = jnp.zeros_like(tri_out)
    load.wait()

    index = lax.broadcasted_iota(jnp.int32, (1, total), 1)
    sub_id = lax.broadcasted_iota(jnp.int32, (PC, 1), 0)
    lane_id = lax.broadcasted_iota(jnp.int32, (PC, LANES), 1)
    group = 32 if rows_here % 32 == 0 else 8
    tiles = cols_here // LANES

    @pl.loop(0, PC)
    def _(j):
        slot = lax.rem(j, 2)
        at_j = lane_id == j
        lower_j = jnp.sum(jnp.where(at_j, lower[:, :LANES], 0.0), axis=1, keepdims=True)
        upper_j = jnp.sum(jnp.where(at_j, upper[:, :LANES], 0.0), axis=1, keepdims=True)
        picked = jnp.where(sub_id == j, panel[...], 0.0)
        column = jnp.sum(
            picked - upper[...] * lower_j - lower[...] * upper_j, axis=0, keepdims=True
        )
        diag = jnp.sum(jnp.where(index == j, column, 0.0), axis=1, keepdims=True)
        lead = jnp.sum(jnp.where(index == j + 1, column, 0.0), axis=1, keepdims=True)
        below = jnp.where(index > j, column, 0.0)
        sigma = jnp.sum(below * below, axis=1, keepdims=True)
        root = jnp.sqrt(sigma)
        alpha = jnp.where(lead >= 0, -root, root)
        length = jnp.sqrt(jnp.maximum(2.0 * (sigma + jnp.abs(lead) * root), 1.0))
        u = (below - jnp.where(index == j + 1, alpha, 0.0)) / length
        unit[...] = jnp.broadcast_to(u, (PC, total))
        tri_out[...] += jnp.where(
            sub_id == j,
            jnp.where(lane_id == 0, diag, jnp.where(lane_id == 1, alpha, 0.0)),
            0.0,
        )
        first = pl.multiple_of(c * cols_here, LANES)

        @pl.loop(0, rows_here // group)
        def _(g):
            acc = [None] * (group // 8)
            for t in range(tiles):
                piece = unit[:, pl.ds(first + t * LANES, LANES)]
                for q in range(group // 8):
                    start = pl.multiple_of(g * group + q * 8, 8)
                    term = block[pl.ds(start, 8), t * LANES:(t + 1) * LANES] * piece
                    acc[q] = term if t == 0 else acc[q] + term
            for q in range(group // 8):
                start = pl.multiple_of(g * group + q * 8, 8)
                sums[pl.ds(start, 8), :] = acc[q]

        partial = lax.dot_general(
            jnp.ones((8, LANES), jnp.float32), sums[...], (((1,), (1,)), ((), ())),
            precision=HIGHEST, preferred_element_type=jnp.float32,
        )
        mine[...] = partial[0:1]
        from_col[slot, c] = partial[0:1]
        copies = [
            pltpu.make_async_remote_copy(
                mine, from_col.at[slot, c], c_send.at[i], c_recv.at[slot, c],
                device_id=(r, peer), device_id_type=MESH,
            )
            for i, peer in enumerate(col_peers)
        ]
        for copy in copies:
            copy.start()
        for peer in col_peers:
            pltpu.make_async_remote_copy(
                mine, from_col.at[slot, peer], c_send.at[0], c_recv.at[slot, peer],
                device_id=(r, peer), device_id_type=MESH,
            ).wait_recv()
        summed = from_col[slot, 0]
        for k in range(1, n_col):
            summed = summed + from_col[slot, k]
        whole_row[...] = summed
        from_row[slot, r] = summed
        row_copies = [
            pltpu.make_async_remote_copy(
                whole_row, from_row.at[slot, r], r_send.at[i], r_recv.at[slot, r],
                device_id=(peer, c), device_id_type=MESH,
            )
            for i, peer in enumerate(row_peers)
        ]
        for copy in row_copies:
            copy.start()
        u_all = unit[...]
        lower_u = jnp.sum(lower[...] * u_all, axis=1, keepdims=True)
        upper_u = jnp.sum(upper[...] * u_all, axis=1, keepdims=True)
        for peer in row_peers:
            pltpu.make_async_remote_copy(
                whole_row, from_row.at[slot, peer], r_send.at[0], r_recv.at[slot, peer],
                device_id=(peer, c), device_id_type=MESH,
            ).wait_recv()
        product = jnp.concatenate([from_row[slot, k] for k in range(n_row)], axis=1)
        image = 2.0 * (
            product
            - jnp.sum(upper[...] * lower_u + lower[...] * upper_u, axis=0, keepdims=True)
        )
        u_row = unit[0:1]
        partner = image - jnp.sum(image * u_row, axis=1, keepdims=True) * u_row
        upper[...] = jnp.where(sub_id == j, unit[...], upper[...])
        lower[...] = jnp.where(sub_id == j, partner, lower[...])
        for copy in copies + row_copies:
            copy.wait_send()

    scale = float(total) ** 0.5
    rows = pl.ds(pl.multiple_of(r * rows_here, LANES), rows_here)
    upper_out[...] = scale * upper[:, rows]
    lower_out[...] = scale * lower[:, rows]


def reduce_panel(casida, n_row, n_col):
    rows_here, cols_here = casida.shape
    total = n_row * rows_here
    f32 = jnp.float32
    dma = pltpu.SemaphoreType.DMA
    vmem = pl.BlockSpec(memory_space=pltpu.VMEM)
    return pl.pallas_call(
        functools.partial(panel_kernel, n_row, n_col),
        out_shape=(
            jax.ShapeDtypeStruct((PC, rows_here), f32),
            jax.ShapeDtypeStruct((PC, rows_here), f32),
            jax.ShapeDtypeStruct((PC, LANES), f32),
        ),
        in_specs=[vmem, pl.BlockSpec(memory_space=pl.ANY)],
        out_specs=(vmem, vmem, vmem),
        scratch_shapes=[
            pltpu.VMEM((rows_here, cols_here), f32),
            pltpu.VMEM((n_col, PC, cols_here), f32),
            pltpu.VMEM((PC, total), f32),
            pltpu.VMEM((PC, total), f32),
            pltpu.VMEM((PC, total), f32),
            pltpu.VMEM((PC, total), f32),
            pltpu.VMEM((rows_here, LANES), f32),
            pltpu.VMEM((1, rows_here), f32),
            pltpu.VMEM((1, rows_here), f32),
            pltpu.VMEM((2, n_col, 1, rows_here), f32),
            pltpu.VMEM((2, n_row, 1, rows_here), f32),
            dma, dma,
            dma((n_row - 1,)), dma,
            dma((n_col - 1,)), dma((n_col,)),
            dma((n_col - 1,)), dma((2, n_col)),
            dma((n_row - 1,)), dma((2, n_row)),
        ],
        compiler_params=pltpu.CompilerParams(
            collective_id=0, has_side_effects=True, vmem_limit_bytes=48 * 1024 * 1024
        ),
    )(casida[:PC], casida)


def shards(pair_factors, k_prev, energies):
    rows_here, cols_here = k_prev.shape
    n_row = lax.axis_size("row")
    n_col = lax.axis_size("col")
    per_col = n_row // n_col
    row_index = lax.axis_index("row")
    col_index = lax.axis_index("col")
    left_rows = lax.all_gather(pair_factors, "col", axis=0, tiled=True)
    moves = []
    for r in range(n_row):
        for c in range(n_col):
            to_row = (r % per_col) * n_col + c
            moves.append((r * n_col + c, to_row * n_col + r // per_col))
    moved = lax.ppermute(pair_factors, ("row", "col"), moves)
    right_rows = lax.all_gather(moved, "row", axis=0, tiled=True)
    product = lax.dot_general(
        left_rows,
        right_rows,
        (((1,), (1,)), ((), ())),
        precision=lax.Precision.HIGH,
        preferred_element_type=jnp.float32,
    )
    global_rows = row_index * rows_here + jnp.arange(rows_here, dtype=jnp.int32)
    global_cols = col_index * cols_here + jnp.arange(cols_here, dtype=jnp.int32)
    on_diagonal = global_rows[:, None] == global_cols[None, :]
    casida = 4.0 * (k_prev + product) + jnp.where(on_diagonal, energies[:, None], 0.0)
    upper, lower, tri = reduce_panel(casida, n_row, n_col)
    return (casida, upper.T, lower.T, tri[:, :2].T)


def solution(mesh):
    in_specs = (P(("row", "col"), None), P("row", "col"), P("row"))
    out_specs = (P("row", "col"), P("row", None), P("row", None), P())
    return jax.shard_map(shards, mesh=mesh, in_specs=in_specs, out_specs=out_specs, check_vma=False)
```

```python
import functools

import jax
import jax.numpy as jnp
from jax import lax
from jax.experimental import pallas as pl
from jax.experimental.pallas import tpu as pltpu
from jax.sharding import PartitionSpec as P

PC = 8
LANES = 128
MESH = pl.DeviceIdType.MESH
HIGHEST = lax.Precision.HIGHEST


def panel_kernel(
    n_row, n_col, part_ref, casida_ref, upper_out, lower_out, tri_out,
    block, panel_in, panel, upper, lower, unit, sums, mine, whole_row, from_col, from_row,
    load_sem, own_sem, pa_send, pa_recv, pb_send, pb_recv, c_send, c_recv, r_send, r_recv,
):
    r = lax.axis_index("row")
    c = lax.axis_index("col")
    rows_here, cols_here = block.shape
    total = n_row * rows_here
    load = pltpu.make_async_copy(casida_ref, block, load_sem)
    load.start()
    col_peers = [lax.rem(c + d, n_col) for d in range(1, n_col)]
    row_peers = [lax.rem(r + d, n_row) for d in range(1, n_row)]
    barrier = pltpu.get_barrier_semaphore()
    for peer in col_peers:
        pl.semaphore_signal(barrier, inc=1, device_id=(r, peer), device_id_type=MESH)
    for peer in row_peers:
        pl.semaphore_signal(barrier, inc=1, device_id=(peer, c), device_id_type=MESH)
    pl.semaphore_wait(barrier, n_col + n_row - 2)

    @pl.when(r == 0)
    def _():
        own = pltpu.make_async_copy(part_ref, panel_in.at[c], own_sem)
        own.start()
        copies = [
            pltpu.make_async_remote_copy(
                part_ref, panel_in.at[c], pa_send.at[d - 1], pa_recv,
                device_id=(jnp.int32(d), c), device_id_type=MESH,
            )
            for d in range(1, n_row)
        ]
        for copy in copies:
            copy.start()
        for copy in copies:
            copy.wait_send()
        own.wait()

    @pl.when(r != 0)
    def _():
        pltpu.make_async_remote_copy(
            part_ref, panel_in.at[c], pa_send.at[0], pa_recv,
            device_id=(jnp.int32(0), c), device_id_type=MESH,
        ).wait_recv()

    copies = [
        pltpu.make_async_remote_copy(
            panel_in.at[c], panel_in.at[c], pb_send.at[i], pb_recv.at[c],
            device_id=(r, peer), device_id_type=MESH,
        )
        for i, peer in enumerate(col_peers)
    ]
    for copy in copies:
        copy.start()
    for peer in col_peers:
        pltpu.make_async_remote_copy(
            panel_in.at[peer], panel_in.at[peer], pb_send.at[0], pb_recv.at[peer],
            device_id=(r, peer), device_id_type=MESH,
        ).wait_recv()
    for copy in copies:
        copy.wait_send()
    for k in range(n_col):
        panel[:, k * cols_here:(k + 1) * cols_here] = panel_in[k]
    upper[...] = jnp.zeros_like(upper)
    lower[...] = jnp.zeros_like(lower)
    tri_out[...] = jnp.zeros_like(tri_out)
    load.wait()

    index = lax.broadcasted_iota(jnp.int32, (1, total), 1)
    sub_id = lax.broadcasted_iota(jnp.int32, (PC, 1), 0)
    lane_id = lax.broadcasted_iota(jnp.int32, (PC, LANES), 1)
    group = 32 if rows_here % 32 == 0 else 8
    tiles = cols_here // LANES

    @pl.loop(0, PC)
    def _(j):
        slot = lax.rem(j, 2)
        at_j = lane_id == j
        lower_j = jnp.sum(jnp.where(at_j, lower[:, :LANES], 0.0), axis=1, keepdims=True)
        upper_j = jnp.sum(jnp.where(at_j, upper[:, :LANES], 0.0), axis=1, keepdims=True)
        picked = jnp.where(sub_id == j, panel[...], 0.0)
        column = jnp.sum(
            picked - upper[...] * lower_j - lower[...] * upper_j, axis=0, keepdims=True
        )
        diag = jnp.sum(jnp.where(index == j, column, 0.0), axis=1, keepdims=True)
        lead = jnp.sum(jnp.where(index == j + 1, column, 0.0), axis=1, keepdims=True)
        below = jnp.where(index > j, column, 0.0)
        sigma = jnp.sum(below * below, axis=1, keepdims=True)
        root = jnp.sqrt(sigma)
        alpha = jnp.where(lead >= 0, -root, root)
        length = jnp.sqrt(jnp.maximum(2.0 * (sigma + jnp.abs(lead) * root), 1.0))
        u = (below - jnp.where(index == j + 1, alpha, 0.0)) / length
        unit[...] = jnp.broadcast_to(u, (PC, total))
        tri_out[...] += jnp.where(
            sub_id == j,
            jnp.where(lane_id == 0, diag, jnp.where(lane_id == 1, alpha, 0.0)),
            0.0,
        )
        first = pl.multiple_of(c * cols_here, LANES)

        @pl.loop(0, rows_here // group)
        def _(g):
            acc = [None] * (group // 8)
            for t in range(tiles):
                piece = unit[:, pl.ds(first + t * LANES, LANES)]
                for q in range(group // 8):
                    start = pl.multiple_of(g * group + q * 8, 8)
                    term = block[pl.ds(start, 8), t * LANES:(t + 1) * LANES] * piece
                    acc[q] = term if t == 0 else acc[q] + term
            for q in range(group // 8):
                start = pl.multiple_of(g * group + q * 8, 8)
                sums[pl.ds(start, 8), :] = acc[q]

        partial = lax.dot_general(
            jnp.ones((8, LANES), jnp.float32), sums[...], (((1,), (1,)), ((), ())),
            precision=HIGHEST, preferred_element_type=jnp.float32,
        )
        mine[...] = partial[0:1]
        from_col[slot, c] = partial[0:1]
        copies = [
            pltpu.make_async_remote_copy(
                mine, from_col.at[slot, c], c_send.at[i], c_recv.at[slot, c],
                device_id=(r, peer), device_id_type=MESH,
            )
            for i, peer in enumerate(col_peers)
        ]
        for copy in copies:
            copy.start()
        for peer in col_peers:
            pltpu.make_async_remote_copy(
                mine, from_col.at[slot, peer], c_send.at[0], c_recv.at[slot, peer],
                device_id=(r, peer), device_id_type=MESH,
            ).wait_recv()
        summed = from_col[slot, 0]
        for k in range(1, n_col):
            summed = summed + from_col[slot, k]
        whole_row[...] = summed
        from_row[slot, r] = summed
        row_copies = [
            pltpu.make_async_remote_copy(
                whole_row, from_row.at[slot, r], r_send.at[i], r_recv.at[slot, r],
                device_id=(peer, c), device_id_type=MESH,
            )
            for i, peer in enumerate(row_peers)
        ]
        for copy in row_copies:
            copy.start()
        u_all = unit[...]
        lower_u = jnp.sum(lower[...] * u_all, axis=1, keepdims=True)
        upper_u = jnp.sum(upper[...] * u_all, axis=1, keepdims=True)
        for peer in row_peers:
            pltpu.make_async_remote_copy(
                whole_row, from_row.at[slot, peer], r_send.at[0], r_recv.at[slot, peer],
                device_id=(peer, c), device_id_type=MESH,
            ).wait_recv()
        product = jnp.concatenate([from_row[slot, k] for k in range(n_row)], axis=1)
        image = 2.0 * (
            product
            - jnp.sum(upper[...] * lower_u + lower[...] * upper_u, axis=0, keepdims=True)
        )
        u_row = unit[0:1]
        partner = image - jnp.sum(image * u_row, axis=1, keepdims=True) * u_row
        upper[...] = jnp.where(sub_id == j, unit[...], upper[...])
        lower[...] = jnp.where(sub_id == j, partner, lower[...])
        for copy in copies + row_copies:
            copy.wait_send()

    scale = float(total) ** 0.5
    rows = pl.ds(pl.multiple_of(r * rows_here, LANES), rows_here)
    upper_out[...] = scale * upper[:, rows]
    lower_out[...] = scale * lower[:, rows]


def reduce_panel(casida, n_row, n_col):
    rows_here, cols_here = casida.shape
    total = n_row * rows_here
    f32 = jnp.float32
    dma = pltpu.SemaphoreType.DMA
    vmem = pl.BlockSpec(memory_space=pltpu.VMEM)
    return pl.pallas_call(
        functools.partial(panel_kernel, n_row, n_col),
        out_shape=(
            jax.ShapeDtypeStruct((PC, rows_here), f32),
            jax.ShapeDtypeStruct((PC, rows_here), f32),
            jax.ShapeDtypeStruct((PC, LANES), f32),
        ),
        in_specs=[vmem, pl.BlockSpec(memory_space=pl.ANY)],
        out_specs=(vmem, vmem, vmem),
        scratch_shapes=[
            pltpu.VMEM((rows_here, cols_here), f32),
            pltpu.VMEM((n_col, PC, cols_here), f32),
            pltpu.VMEM((PC, total), f32),
            pltpu.VMEM((PC, total), f32),
            pltpu.VMEM((PC, total), f32),
            pltpu.VMEM((PC, total), f32),
            pltpu.VMEM((rows_here, LANES), f32),
            pltpu.VMEM((1, rows_here), f32),
            pltpu.VMEM((1, rows_here), f32),
            pltpu.VMEM((2, n_col, 1, rows_here), f32),
            pltpu.VMEM((2, n_row, 1, rows_here), f32),
            dma, dma,
            dma((n_row - 1,)), dma,
            dma((n_col - 1,)), dma((n_col,)),
            dma((n_col - 1,)), dma((2, n_col)),
            dma((n_row - 1,)), dma((2, n_row)),
        ],
        compiler_params=pltpu.CompilerParams(
            collective_id=0, has_side_effects=True, vmem_limit_bytes=48 * 1024 * 1024
        ),
    )(casida[:PC], casida)


def ring_place(i, count):
    if count == 4:
        return i + (i // 2) * (1 - 2 * (i % 2))
    return i


def gather_kernel(
    n_row, n_col, pieces, own_ref, left, right,
    l_recv, l_send, r_recv, r_send, p_recv, p_send, keep_left, keep_right,
):
    r = lax.axis_index("row")
    c = lax.axis_index("col")
    depth = own_ref.shape[0] // pieces
    chips = n_row // 2
    chip, half = r // 2, r % 2
    turn = 1 - 2 * half
    place, root = ring_place(chip, chips), ring_place(c, chips)
    ahead = 2 * ring_place((place + turn + chips) % chips, chips) + half
    behind = 2 * ring_place((place - turn + chips) % chips, chips) + half
    partner = 2 * chip + 1 - half
    distance = ((place - root) * turn + chips) % chips
    has_up, has_down = c < n_col - 1, c > 0
    is_root, is_last = distance == 0, distance == chips - 1

    barrier = pltpu.get_barrier_semaphore()
    for row in (ahead, behind, partner):
        pl.semaphore_signal(barrier, inc=1, device_id=(row, c), device_id_type=MESH)

    @pl.when(has_up)
    def _():
        pl.semaphore_signal(barrier, inc=1, device_id=(r, c + 1), device_id_type=MESH)

    @pl.when(has_down)
    def _():
        pl.semaphore_signal(barrier, inc=1, device_id=(r, c - 1), device_id_type=MESH)

    pl.semaphore_wait(
        barrier, 3 + has_up.astype(jnp.int32) + has_down.astype(jnp.int32)
    )

    def cut(k):
        return pl.ds(k * depth, depth)

    def source(block, k, own):
        return own_ref.at[cut(k)] if own else left.at[block, cut(k)]

    def along(block, k, own, way):
        return pltpu.make_async_remote_copy(
            source(block, k, own), left.at[block, cut(k)],
            l_send.at[(way + 1) // 2, block, k], l_recv.at[block, k],
            device_id=(r, c + way), device_id_type=MESH,
        )

    def spread(block, k, src, to, send, recv):
        return pltpu.make_async_remote_copy(
            src, right.at[half, block, cut(k)], send.at[block, k], recv.at[block, k],
            device_id=(to, c), device_id_type=MESH,
        )

    def root_sends(block, k, own):
        src = source(block, k, own)
        return (
            spread(block, k, src, ahead, r_send, r_recv),
            spread(block, k, src, partner, p_send, p_recv),
            pltpu.make_async_copy(src, right.at[half, block, cut(k)], keep_right.at[block, k]),
        )

    def relay_sends(block, k):
        src = right.at[half, block, cut(k)]
        return (
            spread(block, k, src, ahead, r_send, r_recv),
            spread(block, k, src, partner, p_send, p_recv),
        )

    def from_partner(block, k):
        here = right.at[1 - half, block, cut(k)]
        return pltpu.make_async_remote_copy(
            here, here, p_send.at[block, k], p_recv.at[block, k],
            device_id=(partner, c), device_id_type=MESH,
        )

    def left_event(step, way, k):
        block = c - way * step
        own = step == 0
        ways = (1, -1) if own else (way,)
        if not own:
            along(block, k, False, -way).wait_recv()
        for to in ways:
            @pl.when(has_up if to == 1 else has_down)
            def _():
                along(block, k, own, to).start()

        @pl.when(is_root)
        def _():
            for copy in root_sends(block, k, own):
                copy.start()

    def right_event(step, way, k):
        block = c - way * step

        @pl.when(jnp.logical_not(is_root))
        def _():
            forward, across = relay_sends(block, k)
            forward.wait_recv()
            across.start()

            @pl.when(jnp.logical_not(is_last))
            def _():
                forward.start()

    def finish(step, way, k):
        block = c - way * step
        own = step == 0
        for to in (1, -1) if own else (way,):
            @pl.when(has_up if to == 1 else has_down)
            def _():
                along(block, k, own, to).wait_send()

        from_partner(block, k).wait_recv()

        @pl.when(is_root)
        def _():
            forward, across, keep = root_sends(block, k, own)
            forward.wait_send()
            across.wait_send()
            keep.wait()

        @pl.when(jnp.logical_not(is_root))
        def _():
            forward, across = relay_sends(block, k)
            across.wait_send()

            @pl.when(jnp.logical_not(is_last))
            def _():
                forward.wait_send()

    def guarded(event, step, way, k):
        if step == 0:
            event(step, way, k)
        else:
            @pl.when(c >= step if way == 1 else c + step < n_col)
            def _():
                event(step, way, k)

    events = []
    for step in range(n_col):
        for k in range(pieces):
            for way in (1, -1) if step else (1,):
                events.append((step, way, k))
    lag = 4
    for i in range(len(events) + lag):
        if i < len(events):
            guarded(left_event, *events[i])
        if i == pieces - 1:
            keep = pltpu.make_async_copy(own_ref, left.at[c], keep_left)
            keep.start()
        if i >= lag:
            guarded(right_event, *events[i - lag])
    for event in events:
        guarded(finish, *event)
    keep.wait()


def gather_factors(own, n_row, n_col):
    rows, aux = own.shape
    pieces = 3 if rows % 24 == 0 else 1
    dma = pltpu.SemaphoreType.DMA
    anywhere = pl.BlockSpec(memory_space=pl.ANY)
    per = (n_col, pieces)
    left, right = pl.pallas_call(
        functools.partial(gather_kernel, n_row, n_col, pieces),
        out_shape=(
            jax.ShapeDtypeStruct((n_col, rows, aux), own.dtype),
            jax.ShapeDtypeStruct((2, n_col, rows, aux), own.dtype),
        ),
        in_specs=[anywhere],
        out_specs=(anywhere, anywhere),
        scratch_shapes=[
            dma(per), dma((2,) + per), dma(per), dma(per), dma(per), dma(per),
            dma, dma(per),
        ],
        compiler_params=pltpu.CompilerParams(collective_id=1, has_side_effects=True),
    )(own)
    return left.reshape(n_col * rows, aux), right.reshape(2 * n_col * rows, aux)


def shards(pair_factors, k_prev, energies):
    rows_here, cols_here = k_prev.shape
    n_row = lax.axis_size("row")
    n_col = lax.axis_size("col")
    assert n_row == 2 * n_col
    row_index = lax.axis_index("row")
    col_index = lax.axis_index("col")
    left_rows, right_rows = gather_factors(pair_factors, n_row, n_col)
    product = lax.dot_general(
        left_rows,
        right_rows,
        (((1,), (1,)), ((), ())),
        precision=lax.Precision.HIGH,
        preferred_element_type=jnp.float32,
    )
    global_rows = row_index * rows_here + jnp.arange(rows_here, dtype=jnp.int32)
    global_cols = col_index * cols_here + jnp.arange(cols_here, dtype=jnp.int32)
    on_diagonal = global_rows[:, None] == global_cols[None, :]
    casida = 4.0 * (k_prev + product) + jnp.where(on_diagonal, energies[:, None], 0.0)
    upper, lower, tri = reduce_panel(casida, n_row, n_col)
    return (casida, upper.T, lower.T, tri[:, :2].T)


def solution(mesh):
    in_specs = (P(("row", "col"), None), P("row", "col"), P("row"))
    out_specs = (P("row", "col"), P("row", None), P("row", None), P())
    return jax.shard_map(shards, mesh=mesh, in_specs=in_specs, out_specs=out_specs, check_vma=False)
```

```python
import functools

import jax
import jax.numpy as jnp
from jax import lax
from jax.experimental import pallas as pl
from jax.experimental.pallas import tpu as pltpu
from jax.sharding import PartitionSpec as P

PC = 8
LANES = 128
MESH = pl.DeviceIdType.MESH
HIGHEST = lax.Precision.HIGHEST


def panel_kernel(
    n_row, n_col, part_ref, casida_ref, upper_out, lower_out, tri_out,
    block, panel_in, panel, upper, lower, unit, sums, mine, whole_row, from_col, from_row,
    load_sem, own_sem, pa_send, pa_recv, pb_send, pb_recv, c_send, c_recv, r_send, r_recv,
):
    r = lax.axis_index("row")
    c = lax.axis_index("col")
    rows_here, cols_here = block.shape
    total = n_row * rows_here
    load = pltpu.make_async_copy(casida_ref, block, load_sem)
    load.start()
    col_peers = [lax.rem(c + d, n_col) for d in range(1, n_col)]
    row_peers = [lax.rem(r + d, n_row) for d in range(1, n_row)]
    barrier = pltpu.get_barrier_semaphore()
    for peer in col_peers:
        pl.semaphore_signal(barrier, inc=1, device_id=(r, peer), device_id_type=MESH)
    for peer in row_peers:
        pl.semaphore_signal(barrier, inc=1, device_id=(peer, c), device_id_type=MESH)
    pl.semaphore_wait(barrier, n_col + n_row - 2)

    @pl.when(r == 0)
    def _():
        own = pltpu.make_async_copy(part_ref, panel_in.at[c], own_sem)
        own.start()
        copies = [
            pltpu.make_async_remote_copy(
                part_ref, panel_in.at[c], pa_send.at[d - 1], pa_recv,
                device_id=(jnp.int32(d), c), device_id_type=MESH,
            )
            for d in range(1, n_row)
        ]
        for copy in copies:
            copy.start()
        for copy in copies:
            copy.wait_send()
        own.wait()

    @pl.when(r != 0)
    def _():
        pltpu.make_async_remote_copy(
            part_ref, panel_in.at[c], pa_send.at[0], pa_recv,
            device_id=(jnp.int32(0), c), device_id_type=MESH,
        ).wait_recv()

    copies = [
        pltpu.make_async_remote_copy(
            panel_in.at[c], panel_in.at[c], pb_send.at[i], pb_recv.at[c],
            device_id=(r, peer), device_id_type=MESH,
        )
        for i, peer in enumerate(col_peers)
    ]
    for copy in copies:
        copy.start()
    for peer in col_peers:
        pltpu.make_async_remote_copy(
            panel_in.at[peer], panel_in.at[peer], pb_send.at[0], pb_recv.at[peer],
            device_id=(r, peer), device_id_type=MESH,
        ).wait_recv()
    for copy in copies:
        copy.wait_send()
    for k in range(n_col):
        panel[:, k * cols_here:(k + 1) * cols_here] = panel_in[k]
    upper[...] = jnp.zeros_like(upper)
    lower[...] = jnp.zeros_like(lower)
    tri_out[...] = jnp.zeros_like(tri_out)
    load.wait()

    index = lax.broadcasted_iota(jnp.int32, (1, total), 1)
    sub_id = lax.broadcasted_iota(jnp.int32, (PC, 1), 0)
    lane_id = lax.broadcasted_iota(jnp.int32, (PC, LANES), 1)
    group = 32 if rows_here % 32 == 0 else 8
    tiles = cols_here // LANES

    @pl.loop(0, PC)
    def _(j):
        slot = lax.rem(j, 2)
        at_j = lane_id == j
        lower_j = jnp.sum(jnp.where(at_j, lower[:, :LANES], 0.0), axis=1, keepdims=True)
        upper_j = jnp.sum(jnp.where(at_j, upper[:, :LANES], 0.0), axis=1, keepdims=True)
        picked = jnp.where(sub_id == j, panel[...], 0.0)
        column = jnp.sum(
            picked - upper[...] * lower_j - lower[...] * upper_j, axis=0, keepdims=True
        )
        diag = jnp.sum(jnp.where(index == j, column, 0.0), axis=1, keepdims=True)
        lead = jnp.sum(jnp.where(index == j + 1, column, 0.0), axis=1, keepdims=True)
        below = jnp.where(index > j, column, 0.0)
        sigma = jnp.sum(below * below, axis=1, keepdims=True)
        root = jnp.sqrt(sigma)
        alpha = jnp.where(lead >= 0, -root, root)
        length = jnp.sqrt(jnp.maximum(2.0 * (sigma + jnp.abs(lead) * root), 1.0))
        u = (below - jnp.where(index == j + 1, alpha, 0.0)) / length
        unit[...] = jnp.broadcast_to(u, (PC, total))
        tri_out[...] += jnp.where(
            sub_id == j,
            jnp.where(lane_id == 0, diag, jnp.where(lane_id == 1, alpha, 0.0)),
            0.0,
        )
        first = pl.multiple_of(c * cols_here, LANES)

        @pl.loop(0, rows_here // group)
        def _(g):
            acc = [None] * (group // 8)
            for t in range(tiles):
                piece = unit[:, pl.ds(first + t * LANES, LANES)]
                for q in range(group // 8):
                    start = pl.multiple_of(g * group + q * 8, 8)
                    term = block[pl.ds(start, 8), t * LANES:(t + 1) * LANES] * piece
                    acc[q] = term if t == 0 else acc[q] + term
            for q in range(group // 8):
                start = pl.multiple_of(g * group + q * 8, 8)
                sums[pl.ds(start, 8), :] = acc[q]

        partial = lax.dot_general(
            jnp.ones((8, LANES), jnp.float32), sums[...], (((1,), (1,)), ((), ())),
            precision=HIGHEST, preferred_element_type=jnp.float32,
        )
        mine[...] = partial[0:1]
        from_col[slot, c] = partial[0:1]
        copies = [
            pltpu.make_async_remote_copy(
                mine, from_col.at[slot, c], c_send.at[i], c_recv.at[slot, c],
                device_id=(r, peer), device_id_type=MESH,
            )
            for i, peer in enumerate(col_peers)
        ]
        for copy in copies:
            copy.start()
        for peer in col_peers:
            pltpu.make_async_remote_copy(
                mine, from_col.at[slot, peer], c_send.at[0], c_recv.at[slot, peer],
                device_id=(r, peer), device_id_type=MESH,
            ).wait_recv()
        summed = from_col[slot, 0]
        for k in range(1, n_col):
            summed = summed + from_col[slot, k]
        whole_row[...] = summed
        from_row[slot, r] = summed
        row_copies = [
            pltpu.make_async_remote_copy(
                whole_row, from_row.at[slot, r], r_send.at[i], r_recv.at[slot, r],
                device_id=(peer, c), device_id_type=MESH,
            )
            for i, peer in enumerate(row_peers)
        ]
        for copy in row_copies:
            copy.start()
        u_all = unit[...]
        lower_u = jnp.sum(lower[...] * u_all, axis=1, keepdims=True)
        upper_u = jnp.sum(upper[...] * u_all, axis=1, keepdims=True)
        for peer in row_peers:
            pltpu.make_async_remote_copy(
                whole_row, from_row.at[slot, peer], r_send.at[0], r_recv.at[slot, peer],
                device_id=(peer, c), device_id_type=MESH,
            ).wait_recv()
        product = jnp.concatenate([from_row[slot, k] for k in range(n_row)], axis=1)
        image = 2.0 * (
            product
            - jnp.sum(upper[...] * lower_u + lower[...] * upper_u, axis=0, keepdims=True)
        )
        u_row = unit[0:1]
        partner = image - jnp.sum(image * u_row, axis=1, keepdims=True) * u_row
        upper[...] = jnp.where(sub_id == j, unit[...], upper[...])
        lower[...] = jnp.where(sub_id == j, partner, lower[...])
        for copy in copies + row_copies:
            copy.wait_send()

    scale = float(total) ** 0.5
    rows = pl.ds(pl.multiple_of(r * rows_here, LANES), rows_here)
    upper_out[...] = scale * upper[:, rows]
    lower_out[...] = scale * lower[:, rows]


def reduce_panel(casida, n_row, n_col):
    rows_here, cols_here = casida.shape
    total = n_row * rows_here
    f32 = jnp.float32
    dma = pltpu.SemaphoreType.DMA
    vmem = pl.BlockSpec(memory_space=pltpu.VMEM)
    return pl.pallas_call(
        functools.partial(panel_kernel, n_row, n_col),
        out_shape=(
            jax.ShapeDtypeStruct((PC, rows_here), f32),
            jax.ShapeDtypeStruct((PC, rows_here), f32),
            jax.ShapeDtypeStruct((PC, LANES), f32),
        ),
        in_specs=[vmem, pl.BlockSpec(memory_space=pl.ANY)],
        out_specs=(vmem, vmem, vmem),
        scratch_shapes=[
            pltpu.VMEM((rows_here, cols_here), f32),
            pltpu.VMEM((n_col, PC, cols_here), f32),
            pltpu.VMEM((PC, total), f32),
            pltpu.VMEM((PC, total), f32),
            pltpu.VMEM((PC, total), f32),
            pltpu.VMEM((PC, total), f32),
            pltpu.VMEM((rows_here, LANES), f32),
            pltpu.VMEM((1, rows_here), f32),
            pltpu.VMEM((1, rows_here), f32),
            pltpu.VMEM((2, n_col, 1, rows_here), f32),
            pltpu.VMEM((2, n_row, 1, rows_here), f32),
            dma, dma,
            dma((n_row - 1,)), dma,
            dma((n_col - 1,)), dma((n_col,)),
            dma((n_col - 1,)), dma((2, n_col)),
            dma((n_row - 1,)), dma((2, n_row)),
        ],
        compiler_params=pltpu.CompilerParams(
            collective_id=0, has_side_effects=True, vmem_limit_bytes=48 * 1024 * 1024
        ),
    )(casida[:PC], casida)


def ring_place(i, count):
    if count == 4:
        return i + (i // 2) * (1 - 2 * (i % 2))
    return i


def gather_kernel(
    n_row, n_col, pieces, own_ref, left, right,
    l_recv, l_send, r_recv, r_send, p_recv, p_send, back_send, keep_left,
):
    r = lax.axis_index("row")
    c = lax.axis_index("col")
    depth = own_ref.shape[0] // pieces
    chips = n_row // 2
    chip, half = r // 2, r % 2
    turn = 1 - 2 * half
    place, root = ring_place(chip, chips), ring_place(c, chips)
    ahead = 2 * ring_place((place + turn + chips) % chips, chips) + half
    behind = 2 * ring_place((place - turn + chips) % chips, chips) + half
    partner = 2 * chip + 1 - half
    distance = ((place - root) * turn + chips) % chips
    has_up, has_down = c < n_col - 1, c > 0
    is_root, is_last = distance == 0, distance == chips - 1

    barrier = pltpu.get_barrier_semaphore()
    for row in (ahead, behind, partner):
        pl.semaphore_signal(barrier, inc=1, device_id=(row, c), device_id_type=MESH)

    @pl.when(has_up)
    def _():
        pl.semaphore_signal(barrier, inc=1, device_id=(r, c + 1), device_id_type=MESH)

    @pl.when(has_down)
    def _():
        pl.semaphore_signal(barrier, inc=1, device_id=(r, c - 1), device_id_type=MESH)

    pl.semaphore_wait(
        barrier, 3 + has_up.astype(jnp.int32) + has_down.astype(jnp.int32)
    )

    def cut(k):
        return pl.ds(k * depth, depth)

    def source(block, k, own):
        return own_ref.at[cut(k)] if own else left.at[block, cut(k)]

    def along(block, k, own, way):
        return pltpu.make_async_remote_copy(
            source(block, k, own), left.at[block, cut(k)],
            l_send.at[(way + 1) // 2, block, k], l_recv.at[block, k],
            device_id=(r, c + way), device_id_type=MESH,
        )

    def spread(block, k, src, to, send, recv):
        return pltpu.make_async_remote_copy(
            src, right.at[half, block, cut(k)], send.at[block, k], recv.at[block, k],
            device_id=(to, c), device_id_type=MESH,
        )

    def root_sends(block, k, own):
        src = source(block, k, own)
        return (
            spread(block, k, src, ahead, r_send, r_recv),
            spread(block, k, src, partner, p_send, p_recv),
        )

    def give_back(block, k):
        there = right.at[1 - half, block, cut(k)]
        return pltpu.make_async_remote_copy(
            there, there, back_send.at[block, k], r_recv.at[block, k],
            device_id=(partner, c), device_id_type=MESH,
        )

    def relay_sends(block, k):
        src = right.at[half, block, cut(k)]
        return (
            spread(block, k, src, ahead, r_send, r_recv),
            spread(block, k, src, partner, p_send, p_recv),
        )

    def from_partner(block, k):
        here = right.at[1 - half, block, cut(k)]
        return pltpu.make_async_remote_copy(
            here, here, p_send.at[block, k], p_recv.at[block, k],
            device_id=(partner, c), device_id_type=MESH,
        )

    def left_event(step, way, k):
        block = c - way * step
        own = step == 0
        ways = (1, -1) if own else (way,)
        if not own:
            along(block, k, False, -way).wait_recv()
        for to in ways:
            @pl.when(has_up if to == 1 else has_down)
            def _():
                along(block, k, own, to).start()

        @pl.when(is_root)
        def _():
            for copy in root_sends(block, k, own):
                copy.start()

    def right_event(step, way, k):
        block = c - way * step

        @pl.when(jnp.logical_not(is_root))
        def _():
            forward, across = relay_sends(block, k)
            forward.wait_recv()
            across.start()

            @pl.when(jnp.logical_not(is_last))
            def _():
                forward.start()

    def back_event(step, way, k):
        block = c - way * step

        @pl.when(is_root)
        def _():
            from_partner(block, k).wait_recv()
            give_back(block, k).start()

    def finish(step, way, k):
        block = c - way * step
        own = step == 0
        for to in (1, -1) if own else (way,):
            @pl.when(has_up if to == 1 else has_down)
            def _():
                along(block, k, own, to).wait_send()

        @pl.when(is_root)
        def _():
            forward, across = root_sends(block, k, own)
            forward.wait_send()
            across.wait_send()
            back = give_back(block, k)
            back.wait_send()
            forward.wait_recv()

        @pl.when(jnp.logical_not(is_root))
        def _():
            from_partner(block, k).wait_recv()
            forward, across = relay_sends(block, k)
            across.wait_send()

            @pl.when(jnp.logical_not(is_last))
            def _():
                forward.wait_send()

    def guarded(event, step, way, k):
        if step == 0:
            event(step, way, k)
        else:
            @pl.when(c >= step if way == 1 else c + step < n_col)
            def _():
                event(step, way, k)

    events = []
    for step in range(n_col):
        for k in range(pieces):
            for way in (1, -1) if step else (1,):
                events.append((step, way, k))
    lag = 4
    for i in range(len(events) + lag):
        if i < len(events):
            guarded(left_event, *events[i])
        if i == pieces - 1:
            keep = pltpu.make_async_copy(own_ref, left.at[c], keep_left)
            keep.start()
        if i >= lag:
            guarded(right_event, *events[i - lag])
            guarded(back_event, *events[i - lag])
    for event in events:
        guarded(finish, *event)
    keep.wait()


def gather_factors(own, n_row, n_col):
    rows, aux = own.shape
    pieces = 4 if rows % 32 == 0 else 1
    dma = pltpu.SemaphoreType.DMA
    anywhere = pl.BlockSpec(memory_space=pl.ANY)
    per = (n_col, pieces)
    left, right = pl.pallas_call(
        functools.partial(gather_kernel, n_row, n_col, pieces),
        out_shape=(
            jax.ShapeDtypeStruct((n_col, rows, aux), own.dtype),
            jax.ShapeDtypeStruct((2, n_col, rows, aux), own.dtype),
        ),
        in_specs=[anywhere],
        out_specs=(anywhere, anywhere),
        scratch_shapes=[
            dma(per), dma((2,) + per), dma(per), dma(per), dma(per), dma(per),
            dma(per), dma,
        ],
        compiler_params=pltpu.CompilerParams(collective_id=1, has_side_effects=True),
    )(own)
    return left.reshape(n_col * rows, aux), right.reshape(2 * n_col * rows, aux)


def shards(pair_factors, k_prev, energies):
    rows_here, cols_here = k_prev.shape
    n_row = lax.axis_size("row")
    n_col = lax.axis_size("col")
    assert n_row == 2 * n_col
    row_index = lax.axis_index("row")
    col_index = lax.axis_index("col")
    left_rows, right_rows = gather_factors(pair_factors, n_row, n_col)
    product = lax.dot_general(
        left_rows,
        right_rows,
        (((1,), (1,)), ((), ())),
        precision=lax.Precision.HIGH,
        preferred_element_type=jnp.float32,
    )
    global_rows = row_index * rows_here + jnp.arange(rows_here, dtype=jnp.int32)
    global_cols = col_index * cols_here + jnp.arange(cols_here, dtype=jnp.int32)
    on_diagonal = global_rows[:, None] == global_cols[None, :]
    casida = 4.0 * (k_prev + product) + jnp.where(on_diagonal, energies[:, None], 0.0)
    upper, lower, tri = reduce_panel(casida, n_row, n_col)
    return (casida, upper.T, lower.T, tri[:, :2].T)


def solution(mesh):
    in_specs = (P(("row", "col"), None), P("row", "col"), P("row"))
    out_specs = (P("row", "col"), P("row", None), P("row", None), P())
    return jax.shard_map(shards, mesh=mesh, in_specs=in_specs, out_specs=out_specs, check_vma=False)
```

```python
import functools

import jax
import jax.numpy as jnp
from jax import lax
from jax.experimental import pallas as pl
from jax.experimental.pallas import tpu as pltpu
from jax.sharding import PartitionSpec as P

PC = 8
LANES = 128
MESH = pl.DeviceIdType.MESH
HIGHEST = lax.Precision.HIGHEST


def panel_kernel(
    n_row, n_col, part_ref, casida_ref, upper_out, lower_out, tri_out,
    block, panel_in, panel, upper, lower, unit, sums, mine, whole_row, from_col, from_row,
    load_sem, own_sem, pa_send, pa_recv, pb_send, pb_recv, c_send, c_recv, r_send, r_recv,
):
    r = lax.axis_index("row")
    c = lax.axis_index("col")
    rows_here, cols_here = block.shape
    total = n_row * rows_here
    load = pltpu.make_async_copy(casida_ref, block, load_sem)
    load.start()
    col_peers = [lax.rem(c + d, n_col) for d in range(1, n_col)]
    row_peers = [lax.rem(r + d, n_row) for d in range(1, n_row)]
    barrier = pltpu.get_barrier_semaphore()
    for peer in col_peers:
        pl.semaphore_signal(barrier, inc=1, device_id=(r, peer), device_id_type=MESH)
    for peer in row_peers:
        pl.semaphore_signal(barrier, inc=1, device_id=(peer, c), device_id_type=MESH)
    pl.semaphore_wait(barrier, n_col + n_row - 2)

    @pl.when(r == 0)
    def _():
        own = pltpu.make_async_copy(part_ref, panel_in.at[c], own_sem)
        own.start()
        copies = [
            pltpu.make_async_remote_copy(
                part_ref, panel_in.at[c], pa_send.at[d - 1], pa_recv,
                device_id=(jnp.int32(d), c), device_id_type=MESH,
            )
            for d in range(1, n_row)
        ]
        for copy in copies:
            copy.start()
        for copy in copies:
            copy.wait_send()
        own.wait()

    @pl.when(r != 0)
    def _():
        pltpu.make_async_remote_copy(
            part_ref, panel_in.at[c], pa_send.at[0], pa_recv,
            device_id=(jnp.int32(0), c), device_id_type=MESH,
        ).wait_recv()

    copies = [
        pltpu.make_async_remote_copy(
            panel_in.at[c], panel_in.at[c], pb_send.at[i], pb_recv.at[c],
            device_id=(r, peer), device_id_type=MESH,
        )
        for i, peer in enumerate(col_peers)
    ]
    for copy in copies:
        copy.start()
    for peer in col_peers:
        pltpu.make_async_remote_copy(
            panel_in.at[peer], panel_in.at[peer], pb_send.at[0], pb_recv.at[peer],
            device_id=(r, peer), device_id_type=MESH,
        ).wait_recv()
    for copy in copies:
        copy.wait_send()
    for k in range(n_col):
        panel[:, k * cols_here:(k + 1) * cols_here] = panel_in[k]
    upper[...] = jnp.zeros_like(upper)
    lower[...] = jnp.zeros_like(lower)
    tri_out[...] = jnp.zeros_like(tri_out)
    load.wait()

    index = lax.broadcasted_iota(jnp.int32, (1, total), 1)
    sub_id = lax.broadcasted_iota(jnp.int32, (PC, 1), 0)
    lane_id = lax.broadcasted_iota(jnp.int32, (PC, LANES), 1)
    group = 32 if rows_here % 32 == 0 else 8
    tiles = cols_here // LANES

    @pl.loop(0, PC)
    def _(j):
        slot = lax.rem(j, 2)
        at_j = lane_id == j
        lower_j = jnp.sum(jnp.where(at_j, lower[:, :LANES], 0.0), axis=1, keepdims=True)
        upper_j = jnp.sum(jnp.where(at_j, upper[:, :LANES], 0.0), axis=1, keepdims=True)
        picked = jnp.where(sub_id == j, panel[...], 0.0)
        column = jnp.sum(
            picked - upper[...] * lower_j - lower[...] * upper_j, axis=0, keepdims=True
        )
        diag = jnp.sum(jnp.where(index == j, column, 0.0), axis=1, keepdims=True)
        lead = jnp.sum(jnp.where(index == j + 1, column, 0.0), axis=1, keepdims=True)
        below = jnp.where(index > j, column, 0.0)
        sigma = jnp.sum(below * below, axis=1, keepdims=True)
        root = jnp.sqrt(sigma)
        alpha = jnp.where(lead >= 0, -root, root)
        length = jnp.sqrt(jnp.maximum(2.0 * (sigma + jnp.abs(lead) * root), 1.0))
        u = (below - jnp.where(index == j + 1, alpha, 0.0)) / length
        unit[...] = jnp.broadcast_to(u, (PC, total))
        tri_out[...] += jnp.where(
            sub_id == j,
            jnp.where(lane_id == 0, diag, jnp.where(lane_id == 1, alpha, 0.0)),
            0.0,
        )
        first = pl.multiple_of(c * cols_here, LANES)

        @pl.loop(0, rows_here // group)
        def _(g):
            acc = [None] * (group // 8)
            for t in range(tiles):
                piece = unit[:, pl.ds(first + t * LANES, LANES)]
                for q in range(group // 8):
                    start = pl.multiple_of(g * group + q * 8, 8)
                    term = block[pl.ds(start, 8), t * LANES:(t + 1) * LANES] * piece
                    acc[q] = term if t == 0 else acc[q] + term
            for q in range(group // 8):
                start = pl.multiple_of(g * group + q * 8, 8)
                sums[pl.ds(start, 8), :] = acc[q]

        partial = lax.dot_general(
            jnp.ones((8, LANES), jnp.float32), sums[...], (((1,), (1,)), ((), ())),
            precision=HIGHEST, preferred_element_type=jnp.float32,
        )
        mine[...] = partial[0:1]
        from_col[slot, c] = partial[0:1]
        copies = [
            pltpu.make_async_remote_copy(
                mine, from_col.at[slot, c], c_send.at[i], c_recv.at[slot, c],
                device_id=(r, peer), device_id_type=MESH,
            )
            for i, peer in enumerate(col_peers)
        ]
        for copy in copies:
            copy.start()
        for peer in col_peers:
            pltpu.make_async_remote_copy(
                mine, from_col.at[slot, peer], c_send.at[0], c_recv.at[slot, peer],
                device_id=(r, peer), device_id_type=MESH,
            ).wait_recv()
        summed = from_col[slot, 0]
        for k in range(1, n_col):
            summed = summed + from_col[slot, k]
        whole_row[...] = summed
        from_row[slot, r] = summed
        row_copies = [
            pltpu.make_async_remote_copy(
                whole_row, from_row.at[slot, r], r_send.at[i], r_recv.at[slot, r],
                device_id=(peer, c), device_id_type=MESH,
            )
            for i, peer in enumerate(row_peers)
        ]
        for copy in row_copies:
            copy.start()
        u_all = unit[...]
        lower_u = jnp.sum(lower[...] * u_all, axis=1, keepdims=True)
        upper_u = jnp.sum(upper[...] * u_all, axis=1, keepdims=True)
        for peer in row_peers:
            pltpu.make_async_remote_copy(
                whole_row, from_row.at[slot, peer], r_send.at[0], r_recv.at[slot, peer],
                device_id=(peer, c), device_id_type=MESH,
            ).wait_recv()
        product = jnp.concatenate([from_row[slot, k] for k in range(n_row)], axis=1)
        image = 2.0 * (
            product
            - jnp.sum(upper[...] * lower_u + lower[...] * upper_u, axis=0, keepdims=True)
        )
        u_row = unit[0:1]
        partner = image - jnp.sum(image * u_row, axis=1, keepdims=True) * u_row
        upper[...] = jnp.where(sub_id == j, unit[...], upper[...])
        lower[...] = jnp.where(sub_id == j, partner, lower[...])
        for copy in copies + row_copies:
            copy.wait_send()

    scale = float(total) ** 0.5
    rows = pl.ds(pl.multiple_of(r * rows_here, LANES), rows_here)
    upper_out[...] = scale * upper[:, rows]
    lower_out[...] = scale * lower[:, rows]


def reduce_panel(casida, n_row, n_col):
    rows_here, cols_here = casida.shape
    total = n_row * rows_here
    f32 = jnp.float32
    dma = pltpu.SemaphoreType.DMA
    vmem = pl.BlockSpec(memory_space=pltpu.VMEM)
    return pl.pallas_call(
        functools.partial(panel_kernel, n_row, n_col),
        out_shape=(
            jax.ShapeDtypeStruct((PC, rows_here), f32),
            jax.ShapeDtypeStruct((PC, rows_here), f32),
            jax.ShapeDtypeStruct((PC, LANES), f32),
        ),
        in_specs=[vmem, pl.BlockSpec(memory_space=pl.ANY)],
        out_specs=(vmem, vmem, vmem),
        scratch_shapes=[
            pltpu.VMEM((rows_here, cols_here), f32),
            pltpu.VMEM((n_col, PC, cols_here), f32),
            pltpu.VMEM((PC, total), f32),
            pltpu.VMEM((PC, total), f32),
            pltpu.VMEM((PC, total), f32),
            pltpu.VMEM((PC, total), f32),
            pltpu.VMEM((rows_here, LANES), f32),
            pltpu.VMEM((1, rows_here), f32),
            pltpu.VMEM((1, rows_here), f32),
            pltpu.VMEM((2, n_col, 1, rows_here), f32),
            pltpu.VMEM((2, n_row, 1, rows_here), f32),
            dma, dma,
            dma((n_row - 1,)), dma,
            dma((n_col - 1,)), dma((n_col,)),
            dma((n_col - 1,)), dma((2, n_col)),
            dma((n_row - 1,)), dma((2, n_row)),
        ],
        compiler_params=pltpu.CompilerParams(
            collective_id=0, has_side_effects=True, vmem_limit_bytes=48 * 1024 * 1024
        ),
    )(casida[:PC], casida)


def ring_place(i, count):
    if count == 4:
        return i + (i // 2) * (1 - 2 * (i % 2))
    return i


def gather_kernel(
    n_row, n_col, pieces, own_ref, left, right,
    l_recv, l_send, r_recv, r_send, p_recv, p_send, back_send, keep_left,
):
    r = lax.axis_index("row")
    c = lax.axis_index("col")
    depth = own_ref.shape[0] // pieces
    chips = n_row // 2
    chip, half = r // 2, r % 2
    turn = 1 - 2 * half
    place, root = ring_place(chip, chips), ring_place(c, chips)
    ahead = 2 * ring_place((place + turn + chips) % chips, chips) + half
    behind = 2 * ring_place((place - turn + chips) % chips, chips) + half
    partner = 2 * chip + 1 - half
    distance = ((place - root) * turn + chips) % chips
    has_up, has_down = c < n_col - 1, c > 0
    at_end = jnp.logical_not(has_up & has_down)
    is_root, is_last = distance == 0, distance == chips - 1

    barrier = pltpu.get_barrier_semaphore()
    for row in (ahead, behind, partner):
        pl.semaphore_signal(barrier, inc=1, device_id=(row, c), device_id_type=MESH)

    @pl.when(has_up)
    def _():
        pl.semaphore_signal(barrier, inc=1, device_id=(r, c + 1), device_id_type=MESH)

    @pl.when(has_down)
    def _():
        pl.semaphore_signal(barrier, inc=1, device_id=(r, c - 1), device_id_type=MESH)

    pl.semaphore_wait(
        barrier, 3 + has_up.astype(jnp.int32) + has_down.astype(jnp.int32)
    )

    def cut(k):
        return pl.ds(k * depth, depth)

    def source(block, k, own):
        return own_ref.at[cut(k)] if own else left.at[block, cut(k)]

    def along(block, k, own, way):
        return pltpu.make_async_remote_copy(
            source(block, k, own), left.at[block, cut(k)],
            l_send.at[(way + 1) // 2, block, k], l_recv.at[block, k],
            device_id=(r, c + way), device_id_type=MESH,
        )

    def spread(block, k, src, to, send, recv):
        return pltpu.make_async_remote_copy(
            src, right.at[half, block, cut(k)], send.at[block, k], recv.at[block, k],
            device_id=(to, c), device_id_type=MESH,
        )

    def root_sends(block, k, own):
        src = source(block, k, own)
        return (
            spread(block, k, src, ahead, r_send, r_recv),
            spread(block, k, src, partner, p_send, p_recv),
        )

    def give_back(block, k):
        there = right.at[1 - half, block, cut(k)]
        return pltpu.make_async_remote_copy(
            there, there, back_send.at[block, k], r_recv.at[block, k],
            device_id=(partner, c), device_id_type=MESH,
        )

    def relay_sends(block, k):
        src = right.at[half, block, cut(k)]
        return (
            spread(block, k, src, ahead, r_send, r_recv),
            spread(block, k, src, partner, p_send, p_recv),
        )

    def from_partner(block, k):
        here = right.at[1 - half, block, cut(k)]
        return pltpu.make_async_remote_copy(
            here, here, p_send.at[block, k], p_recv.at[block, k],
            device_id=(partner, c), device_id_type=MESH,
        )

    def left_event(step, way, k):
        block = c - way * step
        own = step == 0
        ways = (1, -1) if own else (way,)
        if not own:
            along(block, k, False, -way).wait_recv()
        for to in ways:
            @pl.when(has_up if to == 1 else has_down)
            def _():
                along(block, k, own, to).start()

        @pl.when(is_root)
        def _():
            for copy in root_sends(block, k, own):
                copy.start()

    def right_event(step, way, k):
        block = c - way * step

        @pl.when(jnp.logical_not(is_root))
        def _():
            forward, across = relay_sends(block, k)
            forward.wait_recv()
            across.start()

            @pl.when(jnp.logical_not(is_last))
            def _():
                forward.start()

    def back_event(step, way, k):
        block = c - way * step

        @pl.when(is_root)
        def _():
            from_partner(block, k).wait_recv()
            give_back(block, k).start()

    def finish(step, way, k):
        block = c - way * step
        own = step == 0
        for to in (1, -1) if own else (way,):
            @pl.when(has_up if to == 1 else has_down)
            def _():
                along(block, k, own, to).wait_send()

        @pl.when(is_root)
        def _():
            forward, across = root_sends(block, k, own)
            forward.wait_send()
            across.wait_send()
            back = give_back(block, k)
            back.wait_send()
            forward.wait_recv()

        @pl.when(jnp.logical_not(is_root))
        def _():
            from_partner(block, k).wait_recv()
            forward, across = relay_sends(block, k)
            across.wait_send()

            @pl.when(jnp.logical_not(is_last))
            def _():
                forward.wait_send()

    def guarded(event, step, way, k):
        if step == 0:
            event(step, way, k)
        else:
            @pl.when(c >= step if way == 1 else c + step < n_col)
            def _():
                event(step, way, k)

    events = []
    for step in range(n_col):
        for k in range(pieces):
            for way in (1, -1) if step else (1,):
                events.append((step, way, k))
    lag = 4
    for i in range(len(events) + lag):
        if i < len(events):
            guarded(left_event, *events[i])
        if i == pieces - 1:
            keep = pltpu.make_async_copy(own_ref, left.at[c], keep_left)
            keep.start()
        soon = range(pieces) if i == pieces else range(i - 1, i) if i > pieces else ()
        for ready, cond in ((soon, at_end), (range(i - lag, i - lag + 1), jnp.logical_not(at_end))):
            for e in ready:
                if 0 <= e < len(events):
                    @pl.when(cond)
                    def _():
                        guarded(right_event, *events[e])
                        guarded(back_event, *events[e])
    for event in events:
        guarded(finish, *event)
    keep.wait()


def gather_factors(own, n_row, n_col):
    rows, aux = own.shape
    pieces = 4 if rows % 32 == 0 else 1
    dma = pltpu.SemaphoreType.DMA
    anywhere = pl.BlockSpec(memory_space=pl.ANY)
    per = (n_col, pieces)
    left, right = pl.pallas_call(
        functools.partial(gather_kernel, n_row, n_col, pieces),
        out_shape=(
            jax.ShapeDtypeStruct((n_col, rows, aux), own.dtype),
            jax.ShapeDtypeStruct((2, n_col, rows, aux), own.dtype),
        ),
        in_specs=[anywhere],
        out_specs=(anywhere, anywhere),
        scratch_shapes=[
            dma(per), dma((2,) + per), dma(per), dma(per), dma(per), dma(per),
            dma(per), dma,
        ],
        compiler_params=pltpu.CompilerParams(collective_id=1, has_side_effects=True),
    )(own)
    return left.reshape(n_col * rows, aux), right.reshape(2 * n_col * rows, aux)


def shards(pair_factors, k_prev, energies):
    rows_here, cols_here = k_prev.shape
    n_row = lax.axis_size("row")
    n_col = lax.axis_size("col")
    assert n_row == 2 * n_col
    row_index = lax.axis_index("row")
    col_index = lax.axis_index("col")
    left_rows, right_rows = gather_factors(pair_factors, n_row, n_col)
    product = lax.dot_general(
        left_rows,
        right_rows,
        (((1,), (1,)), ((), ())),
        precision=lax.Precision.HIGH,
        preferred_element_type=jnp.float32,
    )
    global_rows = row_index * rows_here + jnp.arange(rows_here, dtype=jnp.int32)
    global_cols = col_index * cols_here + jnp.arange(cols_here, dtype=jnp.int32)
    on_diagonal = global_rows[:, None] == global_cols[None, :]
    casida = 4.0 * (k_prev + product) + jnp.where(on_diagonal, energies[:, None], 0.0)
    upper, lower, tri = reduce_panel(casida, n_row, n_col)
    return (casida, upper.T, lower.T, tri[:, :2].T)


def solution(mesh):
    in_specs = (P(("row", "col"), None), P("row", "col"), P("row"))
    out_specs = (P("row", "col"), P("row", None), P("row", None), P())
    return jax.shard_map(shards, mesh=mesh, in_specs=in_specs, out_specs=out_specs, check_vma=False)
```
